32 devices in a mesh: sp: 4 (over x, core), tp: 8 (over z, y).
Axes of the slice: x: 2, y: 2, z: 4, core: 2. Of those that a mesh axis runs over, the one named last changes fastest.
Arguments:
- tokens: bfloat16 [8, 220, 4096], P(None, 'sp'), may hold values from -6 to 6
- modulation: float32 [6, 4096], replicated, may hold values from -2.5 to 2.5
- w_qkv: bfloat16 [4096, 3, 4096], P('sp', None, 'tp'), may hold values from -4 to 4
- w_out: bfloat16 [4096, 4096], P('tp', 'sp'), may hold values from -0.09375 to 0.09375
- w_up: bfloat16 [4096, 16384], P('sp', 'tp'), may hold values from -0.09375 to 0.09375
- w_down: bfloat16 [16384, 4096], P('tp', 'sp'), may hold values from -0.046875 to 0.046875
Outputs:
- block_out: bfloat16 [8, 220, 4096], P(None, 'sp', 'tp')
The draws below stay inside these ranges and needn't reach their ends.
All inputs are finite; a program needn't handle non-finite values.
Results may differ from the reference program's by a relative error of at most 0.012.
Values may be sent and summed in bfloat16 or wider, within the bound.
A program may use at most 128 MiB of HBM per device.

```python
import jax
import jax.numpy as jnp
from jax import lax

D = 4096
HEADS = 32
DH = 128
FF = 16384
FRAMES = 8
PATCHES = 220
N_TP = 8


def draw_w_qkv(key, part):
    inner = HEADS * DH
    base = jax.random.normal(key, (D, 3, inner), jnp.float32) * D ** (-0.5)
    factor = jnp.array([1.3, 1.3, 1.0], jnp.float32)
    base = base * factor[None, :, None]
    base = jnp.clip(base, -4.0, 4.0)
    return base.astype(jnp.bfloat16)


def block_scale(rng, shape, pieces, low, top_value):
    loudness = 1.0
    for axis_at, shards_of in pieces:
        steps = jax.random.uniform(jax.random.fold_in(jax.random.fold_in(rng, 6), axis_at), (shards_of,), jnp.float32, low / len(pieces), top_value / len(pieces))
        loudness = loudness * jnp.repeat(jnp.exp(steps), shape[axis_at] // shards_of).reshape((-1,) + (1,) * (len(shape) - 1 - axis_at))
    return loudness


def normal_values(stream_key, extent, scale, bound, cuts=(), held_as=jnp.bfloat16):
    level = block_scale(stream_key, extent, cuts, -0.22, 0.18) if cuts else 1.0
    drawn = jax.random.normal(stream_key, extent, jnp.float32) * scale * level
    return jnp.minimum(jnp.maximum(drawn, -bound), bound).astype(held_as)


def setup_inputs(seed: int = 0) -> dict:
    keys = jax.random.split(jax.random.key(seed), 7)
    tokens = normal_values(keys[0], (FRAMES, PATCHES, D), 1.0, 6.0, ((1, 4),))
    modulation = normal_values(keys[1], (6, D), 0.5, 2.5, (), jnp.float32)
    w_qkv = draw_w_qkv(jax.random.fold_in(keys[6], 71), 0)
    w_out = normal_values(keys[3], (HEADS * DH, D), (HEADS * DH) ** -0.5, 0.09375, ((0, 8), (1, 4)))
    w_up = normal_values(keys[4], (D, FF), D ** -0.5, 0.09375, ((0, 4), (1, 8)))
    w_down = normal_values(keys[5], (FF, D), FF ** -0.5, 0.046875, ((0, 8), (1, 4)))
    return {"tokens": tokens, "modulation": modulation, "w_qkv": w_qkv, "w_out": w_out, "w_up": w_up, "w_down": w_down}


EPSILON = 1e-06

def normalize(tok_rows, shift_vec, scale_vec):
    values = tok_rows.astype(jnp.float32)
    center = lax.optimization_barrier(jnp.mean(values, axis=-1, keepdims=True))
    spread = lax.optimization_barrier(jnp.mean(jnp.square(values - center), axis=-1, keepdims=True))
    scaled = (values - center) * lax.rsqrt(spread + EPSILON)
    return (scaled * (1.0 + scale_vec) + shift_vec).astype(jnp.bfloat16)

def attend_single(triple):
    query_rows, key_rows, value_rows = triple
    factor = query_rows.shape[-1] ** (-0.5)
    scores = lax.dot_general(query_rows, key_rows, (((1,), (1,)), ((), ())), preferred_element_type=jnp.float32) * factor
    row_max = lax.optimization_barrier(jnp.max(scores, axis=1, keepdims=True))
    raw_weights = jnp.exp(scores - row_max)
    att_weights = (raw_weights / lax.optimization_barrier(jnp.sum(raw_weights, axis=1, keepdims=True))).astype(jnp.bfloat16)
    return jnp.dot(att_weights, value_rows, preferred_element_type=jnp.float32).astype(jnp.bfloat16)

def reference(tokens, modulation, w_qkv, w_out, w_up, w_down):
    frames, patches, width = tokens.shape
    heads_local = HEADS // N_TP
    inner = heads_local * DH
    hidden_local = FF // N_TP
    mod_a = normalize(tokens, modulation[0], modulation[1]).reshape(frames * patches, width)

    def attn_group(group, running):
        begin = (group * inner).astype(jnp.int32)
        weight_group = lax.dynamic_slice_in_dim(w_qkv, begin, inner, 2).reshape(width, 3 * inner)
        projected = jnp.dot(mod_a, weight_group, preferred_element_type=jnp.float32).astype(jnp.bfloat16)
        projected = projected.reshape(frames, patches, 3, heads_local, DH)
        stacked = jnp.transpose(projected, (2, 0, 3, 1, 4)).reshape(3, frames * heads_local, patches, DH)
        attended = lax.map(attend_single, (stacked[0], stacked[1], stacked[2]))
        attended = attended.reshape(frames, heads_local, patches, DH)
        rows_group = lax.dynamic_slice_in_dim(w_out, begin, inner, 0).reshape(heads_local, DH, width)
        term = jnp.einsum('fhpd,hde->fpe', attended.astype(jnp.float32), rows_group.astype(jnp.float32))
        term = lax.optimization_barrier(term.astype(jnp.bfloat16)).astype(jnp.float32)
        return running + term
    attn_sum = lax.fori_loop(0, N_TP, attn_group, jnp.zeros((frames, patches, width), jnp.float32))
    middle = (tokens.astype(jnp.float32) + modulation[2] * attn_sum).astype(jnp.bfloat16)
    mod_b = normalize(middle, modulation[3], modulation[4]).reshape(frames * patches, width)

    def mlp_group(group, running):
        begin = (group * hidden_local).astype(jnp.int32)
        up_cols = lax.dynamic_slice_in_dim(w_up, begin, hidden_local, 1)
        hidden = jax.nn.gelu(jnp.dot(mod_b, up_cols, preferred_element_type=jnp.float32), approximate=True).astype(jnp.bfloat16)
        down_rows = lax.dynamic_slice_in_dim(w_down, begin, hidden_local, 0)
        term = jnp.dot(hidden, down_rows, preferred_element_type=jnp.float32)
        term = lax.optimization_barrier(term.astype(jnp.bfloat16)).astype(jnp.float32)
        return running + term.reshape(frames, patches, width)
    mlp_sum = lax.fori_loop(0, N_TP, mlp_group, jnp.zeros((frames, patches, width), jnp.float32))
    return (middle.astype(jnp.float32) + modulation[5] * mlp_sum).astype(jnp.bfloat16)
```

```python
import math

import jax
import jax.numpy as jnp
from jax import lax
from jax.experimental import pallas as pl
from jax.experimental.pallas import tpu as pltpu
from jax.sharding import PartitionSpec as P

DH = 128
EPSILON = 1e-06
MLP_CHUNKS = 4
BF = jnp.bfloat16
F32 = jnp.float32


def normalize(tok_rows, shift_vec, scale_vec):
    values = tok_rows.astype(F32)
    center = jnp.mean(values, axis=-1, keepdims=True)
    spread = jnp.mean(jnp.square(values - center), axis=-1, keepdims=True)
    scaled = (values - center) * lax.rsqrt(spread + EPSILON)
    return (scaled * (1.0 + scale_vec) + shift_vec).astype(BF)


def reduce_scatter_sp(parts):
    sp_count, n, c = parts.shape
    chips = sp_count // 2
    me = lax.axis_index("sp")
    core, chip = me % 2, me // 2
    pairs = parts.reshape(chips, 2, n, c)
    away = lax.dynamic_index_in_dim(pairs, 1 - core, 1, keepdims=False)
    got = lax.ppermute(away, "sp", [(i, i ^ 1) for i in range(sp_count)])
    mine = lax.dynamic_index_in_dim(pairs, core, 1, keepdims=False)
    both = (mine.astype(F32) + got.astype(F32)).astype(BF)
    total = lax.dynamic_index_in_dim(both, chip, 0, keepdims=False).astype(F32)
    for k in range(1, chips):
        piece = lax.dynamic_index_in_dim(both, (chip + k) % chips, 0, keepdims=False)
        perm = [(i, ((i // 2 + k) % chips) * 2 + i % 2) for i in range(sp_count)]
        total = total + lax.ppermute(piece, "sp", perm).astype(F32)
    return total


def all_gather_sp(piece):
    n, c = piece.shape
    sp_count = lax.axis_size("sp")
    chips = sp_count // 2
    me = lax.axis_index("sp")
    core, chip = me % 2, me // 2
    out = jnp.zeros((chips, 2, n, c), piece.dtype)
    for k in range(chips):
        got = piece
        if k:
            perm = [(i, ((i // 2 + k) % chips) * 2 + i % 2) for i in range(sp_count)]
            got = lax.ppermute(piece, "sp", perm)
        other = lax.ppermute(got, "sp", [(i, i ^ 1) for i in range(sp_count)])
        at = (chip - k) % chips
        out = lax.dynamic_update_slice(out, got[None, None], (at, core, 0, 0))
        out = lax.dynamic_update_slice(out, other[None, None], (at, 1 - core, 0, 0))
    return out.reshape(sp_count, n, c)


def attend(queries, key_rows, values, key_ok):
    factor = queries.shape[-1] ** (-0.5)
    scores = jnp.einsum("iqe,ike->iqk", queries, key_rows, preferred_element_type=F32) * factor
    scores = jnp.where(key_ok, scores, -jnp.inf)
    raw = jnp.exp(scores - jnp.max(scores, axis=-1, keepdims=True))
    att_weights = (raw / jnp.sum(raw, axis=-1, keepdims=True)).astype(BF)
    return jnp.einsum("iqk,ike->iqe", att_weights, values, preferred_element_type=F32).astype(BF)


def shards(tokens, modulation, w_qkv, w_out, w_up, w_down):
    frames, patches, width = tokens.shape
    sp_count, tp_count = lax.axis_size("sp"), lax.axis_size("tp")
    sp_me, tp_me = lax.axis_index("sp"), lax.axis_index("tp")
    heads = w_qkv.shape[2] // DH
    slab = width // sp_count
    groups = math.gcd(frames, tp_count)
    sub, f_own = tp_count // groups, frames // groups
    unit = 8 * sub
    padded = -(-patches // unit) * unit
    part = padded // sub
    rows = sub * sp_count * part
    own_rows = f_own * sp_count * part

    padded_tokens = jnp.pad(tokens, ((0, 0), (0, padded - patches), (0, 0)))
    mine = lax.dynamic_slice(
        padded_tokens, ((tp_me // sub) * f_own, (tp_me % sub) * part, 0), (f_own, part, width)
    )
    mod_mine = normalize(mine, modulation[0], modulation[1])
    def to_slabs(value):
        value = value.reshape(f_own * part, sp_count, slab)
        value = exchange(jnp.transpose(value, (1, 0, 2)), "sp")
        value = value.reshape(sp_count, f_own, part, slab)
        return jnp.transpose(value, (1, 0, 2, 3)).reshape(own_rows, slab)

    mod_slab, tok_slab = to_slabs(mod_mine), to_slabs(mine)
    mod_a = spread_rows(mod_slab, frames, sub, f_own, rows)

    at = jnp.arange(rows)
    key_ok = ((at // (sp_count * part)) * part + at % part) < patches

    chunks = 2 if frames % (2 * sp_count) == 0 else 1
    f_chunk = frames // chunks
    f_split = math.gcd(f_chunk, sp_count)
    h_split = sp_count // f_split
    f_mine, h_mine = f_chunk // f_split, heads // h_split
    w_flat = w_qkv.reshape(slab, 3 * heads * DH)
    attn_parts, att_all = [], []
    fused = tail_fits(frames, rows, heads, w_up.shape[1])
    for c in range(chunks):
        lhs = mod_a[c * f_chunk : (c + 1) * f_chunk].reshape(f_chunk * rows, slab)
        proj = jnp.dot(lhs, w_flat, preferred_element_type=F32).astype(BF)
        if h_split > 1:
            proj = proj.reshape(f_split, f_mine * rows, 3, h_split, h_mine * DH)
            proj = jnp.transpose(proj, (0, 3, 1, 2, 4))
        proj = proj.reshape(sp_count, f_mine * rows, 3 * h_mine * DH)
        proj = reduce_scatter_sp(proj).astype(BF).reshape(f_mine, rows, 3, h_mine, DH)
        proj = jnp.transpose(proj, (2, 0, 3, 1, 4)).reshape(3, f_mine * h_mine, rows, DH)
        att = attend(proj[0], proj[1], proj[2], key_ok)
        att = jnp.transpose(att.reshape(f_mine, h_mine, rows, DH), (0, 2, 1, 3))
        att = all_gather_sp(att.reshape(f_mine * rows, h_mine * DH))
        if h_split > 1:
            att = att.reshape(f_split, h_split, f_mine * rows, h_mine * DH)
            att = jnp.transpose(att, (0, 2, 1, 3))
        att = att.reshape(f_chunk * rows, heads * DH)
        att_all.append(att)
        if fused:
            continue
        attn_parts.append(jnp.dot(att, w_out, preferred_element_type=F32).astype(BF))
    if fused:
        att = jnp.concatenate(att_all, 0)
        mod_slice = lax.dynamic_slice_in_dim(modulation, sp_me * slab, slab, 1)
        block = run_tail(att, tok_slab, mod_slice, w_out, w_up, w_down, frames, part)
        return block[:, :patches]
    attn_part = jnp.concatenate(attn_parts, 0).reshape(tp_count, own_rows, slab)
    attn_sum = reduce_scatter_tp(attn_part)

    mod_slice = lax.dynamic_slice_in_dim(modulation, sp_me * slab, slab, 1)
    middle = (tok_slab.astype(F32) + mod_slice[2] * attn_sum).astype(BF)

    values = middle.astype(F32)
    mean_s = jnp.mean(values, axis=-1)
    dev_s = jnp.sum(jnp.square(values - mean_s[:, None]), axis=-1)
    stats = lax.all_gather(jnp.stack([mean_s, dev_s]), "sp", axis=0)
    center = jnp.mean(stats[:, 0], axis=0)
    spread = (jnp.sum(stats[:, 1], 0) + slab * jnp.sum(jnp.square(stats[:, 0] - center), 0)) / width
    scaled = (values - center[:, None]) * lax.rsqrt(spread + EPSILON)[:, None]
    mod_b = (scaled * (1.0 + mod_slice[4]) + mod_slice[3]).astype(BF)
    mod_b = spread_rows(mod_b, frames, sub, f_own, rows).reshape(frames * rows, slab)

    hid = w_up.shape[1] // MLP_CHUNKS
    share = frames * rows // sp_count
    acc = None
    for c in range(MLP_CHUNKS):
        up = jnp.dot(mod_b, w_up[:, c * hid : (c + 1) * hid], preferred_element_type=F32)
        up = reduce_scatter_sp(up.astype(BF).reshape(sp_count, share, hid))
        hidden = jax.nn.gelu(up, approximate=True).astype(BF)
        hidden = all_gather_sp(hidden).reshape(frames * rows, hid)
        term = jnp.dot(hidden, w_down[c * hid : (c + 1) * hid], preferred_element_type=F32)
        acc = term if acc is None else acc + term
    mlp_part = acc.astype(BF).reshape(tp_count, own_rows, slab)
    mlp_sum = reduce_scatter_tp(mlp_part)
    block = (middle.astype(F32) + mod_slice[5] * mlp_sum).astype(BF)

    block = jnp.transpose(block.reshape(f_own, sp_count, part, slab), (1, 0, 2, 3))
    block = exchange(block.reshape(sp_count, f_own * part, slab), "sp")
    block = jnp.transpose(block, (1, 0, 2)).reshape(f_own * part, tp_count, width // tp_count)
    block = exchange(jnp.transpose(block, (1, 0, 2)), "tp")
    block = block.reshape(groups, sub, f_own, part, width // tp_count)
    block = jnp.transpose(block, (0, 2, 1, 3, 4)).reshape(frames, padded, width // tp_count)
    return block[:, :patches]


def tail_fits(frames, rows, heads, hidden):
    sp_count, tp_count = lax.axis_size("sp"), lax.axis_size("tp")
    _, ring, lanes = tp_grid()
    return (
        sp_count == 4
        and lanes == 2
        and ring > 1
        and tp_count == frames
        and rows % 32 == 0
        and rows <= 256
        and (heads * DH) % 256 == 0
        and hidden % 1024 == 0
    )


def tile_loop(count, body):
    def step(i, carry):
        body(i)
        return carry

    lax.fori_loop(0, count, step, 0)


def tail_kernel(
    att_ref, tok_ref, mod_ref, w_out_ref, w_up_ref, w_down_ref, out_ref,
    wo, wu, wd, part, partm, y_in, z_in, modb, up_out, up_in, up_own, hid, acc, mid, fin, st,
    w_sem, wx_send, wx_recv, y_send, y_recv, z_send, z_recv, st_send, st_recv,
    az_send, az_recv, ay_send, ay_recv, ap_send, ap_recv, u_send, u_recv,
    hx_send, hx_recv, hp_send, hp_recv, hf_send, hf_recv, o_send, o_recv,
):
    sp, tp = lax.axis_index("sp"), lax.axis_index("tp")
    count, ring, lanes = tp_grid()
    core, chip = lax.rem(sp, 2), lax.div(sp, 2)
    z, y = lax.div(tp, lanes), lax.rem(tp, lanes)
    lane = 1 - y
    partner, across = chip * 2 + (1 - core), (1 - chip) * 2 + core
    total, rows, inner = att_ref.shape
    slab = wo.shape[1]
    half, quarter = wu.shape[1], up_out.shape[2]
    width = 4 * slab
    parts, part_rows = fin.shape[0], fin.shape[1]
    lanes_wide = out_ref.shape[2]
    per_slab = slab // lanes_wide
    group = rows // 2

    def rc(src, dst, ssem, rsem, **dev):
        return pltpu.make_async_remote_copy(
            src_ref=src, dst_ref=dst, send_sem=ssem, recv_sem=rsem,
            device_id=dev, device_id_type=pl.DeviceIdType.MESH,
        )

    def near(k):
        low = z < ring // 2
        zz = jnp.where(low, z, ring - 1 - z)
        at = jnp.where(k == 0, zz, jnp.where(k <= zz, k - 1, k))
        return jnp.where(low, at, ring - 1 - at)

    local = [
        pltpu.make_async_copy(w_out_ref, wo, w_sem.at[0]),
        pltpu.make_async_copy(
            w_up_ref.at[:, pl.ds(pl.multiple_of(core * half, 128), half)],
            wu.at[pl.ds(pl.multiple_of(core * slab, 128), slab)],
            w_sem.at[1],
        ),
        pltpu.make_async_copy(w_down_ref, wd, w_sem.at[2]),
    ]
    for c in local:
        c.start()
    swap = rc(
        w_up_ref.at[:, pl.ds(pl.multiple_of((1 - core) * half, 128), half)],
        wu.at[pl.ds(pl.multiple_of(core * slab, 128), slab)],
        wx_send, wx_recv, sp=partner,
    )
    swap.start()
    local[0].wait()

    def y_copy(p, buf, zf):
        return rc(buf.at[zf * lanes + lane], y_in.at[p, zf], y_send.at[p, zf], y_recv.at[p, zf], tp=z * lanes + lane)

    def z_copy(p, buf, zf):
        up = zf > z
        nxt = jnp.where(up, z + 1, z - 1)
        slot = jnp.where(jnp.logical_and(nxt == zf, z > zf), ring, zf)
        return rc(buf.at[zf * lanes + y], z_in.at[p, slot], z_send.at[p, zf], z_recv.at[p, slot], tp=nxt * lanes + y)

    def add_rows(dst, src):
        def body(i):
            at = pl.ds(pl.multiple_of(i * 32, 32), 32)
            dst[at, :] = dst[at, :] + src[at, :].astype(F32)
        tile_loop(rows // 32, body)

    def gather_sum(p, buf, zf):
        y_copy(p, buf, zf).wait_recv()
        f = zf * lanes + y

        def body(i):
            at = pl.ds(pl.multiple_of(i * 32, 32), 32)
            acc[at, :] = buf[f, at, :].astype(F32) + y_in[p, zf, at, :].astype(F32)
        tile_loop(rows // 32, body)

        def take(slot):
            pltpu.make_async_copy(z_in.at[p, slot], z_in.at[p, slot], z_recv.at[p, slot]).wait()
            add_rows(acc, z_in.at[p, slot])

        @pl.when(jnp.logical_and(zf >= z, z > 0))
        def _():
            take(zf)

        @pl.when(jnp.logical_and(zf <= z, z < ring - 1))
        def _():
            take(jnp.where(zf == z, ring, zf))

    def reduce_tp(p, buf):
        def step(k):
            zf = near(ring - 1 - k)
            gather_sum(p, buf, zf)
            f = zf * lanes + y

            @pl.when(zf != z)
            def _():
                def body(i):
                    at = pl.ds(pl.multiple_of(i * 32, 32), 32)
                    buf[f, at, :] = acc[at, :].astype(BF)
                tile_loop(rows // 32, body)
                z_copy(p, buf, zf).start()
        tile_loop(ring, step)

    def reduce_done(p, buf):
        def step(zf):
            y_copy(p, buf, zf).wait_send()

            @pl.when(zf != z)
            def _():
                z_copy(p, buf, zf).wait_send()
        tile_loop(ring, step)

    def project(k):
        zf = near(ring - 1 - k)
        for d in (lane, y):
            f = zf * lanes + d

            def body(n):
                cols = pl.ds(pl.multiple_of(n * 256, 256), 256)
                part[f, :, cols] = jnp.dot(att_ref[f], wo[:, cols], preferred_element_type=F32).astype(BF)
            tile_loop(slab // 256, body)
            if d is lane:
                y_copy(0, part, zf).start()
    tile_loop(ring, project)
    reduce_tp(0, part)

    eye = lax.broadcasted_iota(jnp.int32, (group, 128), 0) == lax.broadcasted_iota(jnp.int32, (group, 128), 1)

    def to_row(col):
        return jnp.sum(jnp.where(eye, col, 0.0), axis=0, keepdims=True)

    def to_col(row):
        return jnp.sum(jnp.where(eye, jnp.broadcast_to(row, (group, 128)), 0.0), axis=1, keepdims=True)

    for g in range(2):
        at = pl.ds(g * group, group)
        value = (tok_ref[at, :].astype(F32) + mod_ref[2:3, :] * acc[at, :]).astype(BF).astype(F32)
        mid[at, :] = value
        mean_s = jnp.sum(value, axis=1, keepdims=True) / slab
        dev_s = jnp.sum(jnp.square(value - mean_s), axis=1, keepdims=True)
        st[sp, pl.ds(g, 1), :] = to_row(mean_s)
        st[sp, pl.ds(2 + g, 1), :] = to_row(dev_s)
    def st_copy(k):
        return rc(st.at[sp], st.at[sp], st_send.at[k - 1], st_recv.at[k - 1], sp=lax.rem(sp + k, 4))
    for k in range(1, 4):
        st_copy(k).start()
    for k in range(1, 4):
        got = lax.rem(sp + 4 - k, 4)
        rc(st.at[got], st.at[got], st_send.at[k - 1], st_recv.at[k - 1], sp=got).wait_recv()
    for g in range(2):
        at = pl.ds(g * group, group)
        means = [st[s, pl.ds(g, 1), :] for s in range(4)]
        devs = [st[s, pl.ds(2 + g, 1), :] for s in range(4)]
        center = (means[0] + means[1] + means[2] + means[3]) / 4
        spread = devs[0] + devs[1] + devs[2] + devs[3]
        for m in means:
            spread = spread + slab * jnp.square(m - center)
        scale = to_col(lax.rsqrt(spread / width + EPSILON))
        value = (mid[at, :] - to_col(center)) * scale
        modb[core, tp, at, :] = (value * (1.0 + mod_ref[4:5, :]) + mod_ref[3:4, :]).astype(BF)

    def az_copy(zs, up):
        f = zs * lanes + y
        nxt = jnp.where(up, z + 1, z - 1)
        side = jnp.where(up, 1, 0)
        return rc(modb.at[core, f], modb.at[core, f], az_send.at[side, zs], az_recv.at[zs], tp=nxt * lanes + y)

    def ay_copy(zs, at_y):
        f = zs * lanes + at_y
        return rc(modb.at[core, f], modb.at[core, f], ay_send.at[zs], ay_recv.at[zs], tp=z * lanes + lane)

    def ap_copy(slab_at, f):
        return rc(modb.at[slab_at, f], modb.at[slab_at, f], ap_send.at[f], ap_recv.at[f], sp=partner)

    def serve(k):
        zs = near(k)

        @pl.when(zs != z)
        def _():
            az_copy(zs, True).wait_recv()

        @pl.when(jnp.logical_and(zs <= z, z < ring - 1))
        def _():
            az_copy(zs, True).start()

        @pl.when(jnp.logical_and(zs >= z, z > 0))
        def _():
            az_copy(zs, False).start()
        ay_copy(zs, y).start()
        ap_copy(core, zs * lanes + y).start()

    def serve_lane(k):
        zs = near(k)
        ay_copy(zs, lane).wait_recv()
        ap_copy(core, zs * lanes + lane).start()

    serve(0)
    local[1].wait()
    swap.wait()
    local[2].wait()

    def piece(i):
        zs = near(lax.div(i, lanes))
        d = lax.rem(i, lanes)
        return zs, jnp.where(d == 0, y, lane)

    def u_copy(f):
        return rc(up_out.at[f], up_in.at[f], u_send.at[f], u_recv.at[f], sp=across)

    def cols_of(who_chip, who_core):
        return pl.ds(pl.multiple_of(who_core * half + who_chip * quarter, 128), quarter)

    def hx_copy(f, who):
        ref = hid.at[f, :, cols_of(who, core)]
        return rc(ref, ref, hx_send.at[f], hx_recv.at[f], sp=across)

    def hp_copy(f, who):
        ref = hid.at[f, :, cols_of(chip, who)]
        return rc(ref, ref, hp_send.at[f], hp_recv.at[f], sp=partner)

    def hf_copy(f, who):
        ref = hid.at[f, :, cols_of(1 - chip, who)]
        return rc(ref, ref, hf_send.at[f], hf_recv.at[f], sp=partner)

    def stage_up(i):
        zs, at_y = piece(i)
        f = zs * lanes + at_y
        ap_copy(1 - core, f).wait_recv()

        def product(col):
            cols = pl.ds(pl.multiple_of(col, 128), 256)
            return jnp.dot(modb[0, f], wu[0:slab, cols], preferred_element_type=F32) + jnp.dot(
                modb[1, f], wu[slab : 2 * slab, cols], preferred_element_type=F32
            )

        def away(n):
            up_out[f, :, pl.ds(pl.multiple_of(n * 256, 256), 256)] = product((1 - chip) * quarter + n * 256).astype(BF)
        tile_loop(quarter // 256, away)
        u_copy(f).start()

        def home(n):
            up_own[lax.rem(i, 2), :, pl.ds(pl.multiple_of(n * 256, 256), 256)] = product(chip * quarter + n * 256)
        tile_loop(quarter // 256, home)

    def stage_gelu(i):
        zs, at_y = piece(i)
        f = zs * lanes + at_y
        u_copy(f).wait_recv()

        def body(j):
            at = pl.ds(pl.multiple_of(j * 32, 32), 32)
            v = up_own[lax.rem(i, 2), at, :] + up_in[f, at, :].astype(F32)
            hid[f, at, cols_of(chip, core)] = jax.nn.gelu(v, approximate=True).astype(BF)
        tile_loop(rows // 32, body)
        hx_copy(f, chip).start()
        hp_copy(f, core).start()

    def stage_forward(i):
        zs, at_y = piece(i)
        f = zs * lanes + at_y
        hx_copy(f, 1 - chip).wait_recv()
        hf_copy(f, core).start()

    def stage_down(i):
        zs, at_y = piece(i)
        f = zs * lanes + at_y
        hp_copy(f, 1 - core).wait_recv()
        hf_copy(f, 1 - core).wait_recv()

        def body(n):
            cols = pl.ds(pl.multiple_of(n * 256, 256), 256)
            partm[f, :, cols] = jnp.dot(hid[f], wd[:, cols], preferred_element_type=F32).astype(BF)
        tile_loop(slab // 256, body)

        @pl.when(at_y == lane)
        def _():
            y_copy(1, partm, zs).start()

    def mlp(i):
        @pl.when(i < total)
        def _():
            stage_up(i)

        @pl.when(jnp.logical_and(i >= 1, i < total + 1))
        def _():
            stage_gelu(i - 1)

        @pl.when(jnp.logical_and(i >= 2, i < total + 2))
        def _():
            stage_forward(i - 2)

        @pl.when(i >= 3)
        def _():
            stage_down(i - 3)

        @pl.when(i + 1 < ring)
        def _():
            serve(i + 1)

        @pl.when(jnp.logical_and(i + 1 < total, lax.rem(i + 1, lanes) != 0))
        def _():
            serve_lane(lax.div(i + 1, lanes))
    tile_loop(total + 3, mlp)
    reduce_tp(1, partm)

    for j in range(parts):
        at = pl.ds(j * part_rows, part_rows)
        fin[j] = (mid[at, :] + mod_ref[5:6, :] * acc[at, :]).astype(BF)

    def o_copy(j, q):
        at = tp * parts + j
        frame, to_sp, to_tp = lax.div(at, 4), lax.rem(at, 4), sp * per_slab + q
        src = fin.at[j, :, pl.ds(q * lanes_wide, lanes_wide)]
        here = jnp.logical_and(to_sp == sp, to_tp == tp)
        far = rc(src, out_ref.at[frame], o_send.at[j * per_slab + q], o_recv.at[frame], sp=to_sp, tp=to_tp)
        near_by = pltpu.make_async_copy(src, out_ref.at[frame], o_recv.at[frame])
        return here, far, near_by

    for j in range(parts):
        for q in range(per_slab):
            here, far, near_by = o_copy(j, q)

            @pl.when(here)
            def _():
                near_by.start()

            @pl.when(jnp.logical_not(here))
            def _():
                far.start()

    for k in range(1, 4):
        st_copy(k).wait_send()
    reduce_done(0, part)
    reduce_done(1, partm)

    def drain(zs):
        @pl.when(jnp.logical_and(zs <= z, z < ring - 1))
        def _():
            az_copy(zs, True).wait_send()

        @pl.when(jnp.logical_and(zs >= z, z > 0))
        def _():
            az_copy(zs, False).wait_send()
        ay_copy(zs, y).wait_send()
    tile_loop(ring, drain)

    def drain_pieces(f):
        ap_copy(core, f).wait_send()
        u_copy(f).wait_send()
        hx_copy(f, chip).wait_send()
        hp_copy(f, core).wait_send()
        hf_copy(f, core).wait_send()
    tile_loop(total, drain_pieces)
    for j in range(parts):
        for q in range(per_slab):
            here, far, _ = o_copy(j, q)

            @pl.when(jnp.logical_not(here))
            def _():
                far.wait_send()
    for frame in range(out_ref.shape[0]):
        pltpu.make_async_copy(out_ref.at[frame], out_ref.at[frame], o_recv.at[frame]).wait()


def run_tail(att, tok_slab, mod_slice, w_out, w_up, w_down, frames, part):
    sp_count, tp_count = lax.axis_size("sp"), lax.axis_size("tp")
    _, ring, lanes = tp_grid()
    total = tp_count
    rows, slab = tok_slab.shape
    inner, hidden = w_out.shape[0], w_up.shape[1]
    half, quarter = hidden // 2, hidden // 4
    parts = rows // part
    wide = sp_count * slab // tp_count
    dma = pltpu.SemaphoreType.DMA
    vm = pl.BlockSpec(memory_space=pltpu.VMEM)
    hbm = pl.BlockSpec(memory_space=pl.ANY)
    flops = 2 * total * rows * slab * (inner + 2 * hidden)
    return pl.pallas_call(
        tail_kernel,
        name="tail",
        out_shape=jax.ShapeDtypeStruct((frames, part, wide), BF),
        in_specs=[vm, vm, vm, hbm, hbm, hbm],
        out_specs=hbm,
        scratch_shapes=[
            pltpu.VMEM((inner, slab), BF),
            pltpu.VMEM((2 * slab, half), BF),
            pltpu.VMEM((hidden, slab), BF),
            pltpu.VMEM((total, rows, slab), BF),
            pltpu.VMEM((total, rows, slab), BF),
            pltpu.VMEM((2, ring, rows, slab), BF),
            pltpu.VMEM((2, ring + 1, rows, slab), BF),
            pltpu.VMEM((2, total, rows, slab), BF),
            pltpu.VMEM((total, rows, quarter), BF),
            pltpu.VMEM((total, rows, quarter), BF),
            pltpu.VMEM((2, rows, quarter), F32),
            pltpu.VMEM((total, rows, hidden), BF),
            pltpu.VMEM((rows, slab), F32),
            pltpu.VMEM((rows, slab), F32),
            pltpu.VMEM((parts, part, slab), BF),
            pltpu.VMEM((4, 8, 128), F32),
            dma((3,)), dma, dma,
            dma((2, ring)), dma((2, ring)),
            dma((2, ring)), dma((2, ring + 1)),
            dma((3,)), dma((3,)),
            dma((2, ring)), dma((ring,)),
            dma((ring,)), dma((ring,)),
            dma((total,)), dma((total,)),
            dma((total,)), dma((total,)),
            dma((total,)), dma((total,)),
            dma((total,)), dma((total,)),
            dma((total,)), dma((total,)),
            dma((parts * (slab // wide),)), dma((frames,)),
        ],
        compiler_params=pltpu.CompilerParams(has_side_effects=True, vmem_limit_bytes=64000000),
        cost_estimate=pl.CostEstimate(flops=flops, bytes_accessed=2 * rows * slab * total, transcendentals=0),
    )(att.reshape(total, rows, inner), tok_slab, mod_slice, w_out, w_up, w_down)


def tp_grid():
    count = lax.axis_size("tp")
    lanes = 2 ** ((count.bit_length() - 1) // 2)
    return count, count // lanes, lanes


def ring_shift(value, k):
    count, ring, lanes = tp_grid()
    return lax.ppermute(
        value, "tp", [(i, ((i // lanes + k) % ring) * lanes + i % lanes) for i in range(count)]
    )


def lane_shift(value, k):
    count, ring, lanes = tp_grid()
    return lax.ppermute(
        value, "tp", [(i, (i // lanes) * lanes + (i + k) % lanes) for i in range(count)]
    )


def ring_pieces(piece):
    ring = tp_grid()[1]
    if ring != 4:
        return [(k, ring_shift(piece, k) if k else piece) for k in range(ring)]
    half = piece.shape[1] // 2
    left, right = ring_shift(piece, 1), ring_shift(piece, -1)
    far = [ring_shift(left[:, :half], 1), ring_shift(right[:, half:], -1)]
    return [(0, piece), (1, left), (3, right), (2, jnp.concatenate(far, 1))]


def ring_reduce(parts):
    ring = parts.shape[0]
    _, _, lanes = tp_grid()
    place = lax.axis_index("tp") // lanes

    def part(k):
        return lax.dynamic_index_in_dim(parts, (place + k) % ring, 0, keepdims=False)

    total = part(0).astype(F32)
    if ring != 4:
        for k in range(1, ring):
            total = total + ring_shift(part(k), k).astype(F32)
        return total
    half = parts.shape[2] // 2
    far = part(2)
    from_left, from_right = ring_shift(far[:, :half], 1), ring_shift(far[:, half:], -1)
    ahead, behind = part(1), part(3)
    low = (ahead[:, :half].astype(F32) + from_left.astype(F32)).astype(BF)
    high = (behind[:, half:].astype(F32) + from_right.astype(F32)).astype(BF)
    ahead = jnp.concatenate([low, ahead[:, half:]], 1)
    behind = jnp.concatenate([behind[:, :half], high], 1)
    return total + ring_shift(ahead, 1).astype(F32) + ring_shift(behind, -1).astype(F32)


def reduce_scatter_tp(parts):
    count, ring, lanes = tp_grid()
    lane = lax.axis_index("tp") % lanes
    grid = parts.reshape((ring, lanes) + parts.shape[1:])
    total = None
    for k in list(range(1, lanes)) + [0]:
        picked = lax.dynamic_index_in_dim(grid, (lane + k) % lanes, 1, keepdims=False)
        summed = ring_reduce(picked)
        if k:
            summed = lane_shift(summed.astype(BF), k).astype(F32)
        total = summed if total is None else total + summed
    return total


def spread_rows(own, frames, sub, f_own, rows):
    count, ring, lanes = tp_grid()
    me = lax.axis_index("tp")
    place, lane = me // lanes, me % lanes
    out = jnp.zeros((count,) + own.shape, own.dtype)
    for k in range(lanes):
        column = lane_shift(own, k) if k else own
        for back, piece in ring_pieces(column):
            at = ((place - back) % ring) * lanes + (lane - k) % lanes
            out = lax.dynamic_update_slice(out, piece[None], (at, 0, 0))
    return out.reshape(frames, rows, own.shape[1])


def exchange(parts, axis):
    count = parts.shape[0]
    me = lax.axis_index(axis)
    out = parts
    for k in range(1, count):
        piece = lax.dynamic_index_in_dim(parts, (me + k) % count, 0)
        got = lax.ppermute(piece, axis, [(i, (i + k) % count) for i in range(count)])
        out = lax.dynamic_update_slice_in_dim(out, got, (me - k) % count, 0)
    return out


def solution(mesh):
    placed = (
        P(None, "sp", None),
        P(),
        P("sp", None, "tp"),
        P("tp", "sp"),
        P("sp", "tp"),
        P("tp", "sp"),
    )
    return jax.shard_map(
        shards, mesh=mesh, in_specs=placed, out_specs=P(None, "sp", "tp"), check_vma=False
    )
```
